32 devices in a mesh: blk: 8 (over z, y), batch: 4 (over x, core).
Axes of the slice: x: 2, y: 2, z: 4, core: 2. Of those that a mesh axis runs over, the one named last changes fastest.
Arguments:
- coefficients: bfloat16 [120, 24576], P(None, ('blk', 'batch')), may hold values from -6 to 6
- transforms: bfloat16 [12, 24, 24576], P(None, 'batch', 'blk'), may hold values from -6 to 6
- basis: bfloat16 [120, 3, 4096], P(None, None, 'blk'), may hold values from -0.5 to 0.5
- template: bfloat16 [3, 4096], P(None, 'blk'), may hold values from -6 to 6
- skin_weights: bfloat16 [24, 4096], P(None, 'blk'), may hold values from 0.019897461 to 1
Outputs:
- skinned: bfloat16 [24576, 4, 3, 512], P(('blk', 'batch'))
The draws below stay inside these ranges and needn't reach their ends.
All inputs are finite; a program needn't handle non-finite values.
Results may differ from the reference program's by a relative error of at most 0.0049.
Values may be sent and summed in bfloat16 or wider, within the bound.
No kernel may reach another device: no remote copies, remote signals or barrier semaphores. Data moves between devices by JAX's collectives and lax.ppermute only.
A program may use at most 192 MiB of HBM per device.

```python
import math
import jax
import jax.numpy as jnp
from jax import lax

K = 120
J = 24
VB = 512
R = 768
STEPS = 4
VERTS = 4096
CHARS = 24576
N_BLK = 8
N_BATCH = 4


def levels(stream_key, dims, pieces, low, top_value):
    def one(axis_at, parts):
        heights = jax.random.uniform(jax.random.fold_in(jax.random.fold_in(stream_key, 6), axis_at), (parts,), jnp.float32, low / len(pieces), top_value / len(pieces))
        return jnp.repeat(jnp.exp(heights), dims[axis_at] // parts).reshape((-1,) + (1,) * (len(dims) - axis_at - 1))

    gain = one(*pieces[0])
    for cut in pieces[1:]:
        gain = gain * one(*cut)
    return gain


def noise(rng, extent, spread, reach, pieces=(), held_as=jnp.bfloat16):
    entries = jax.random.normal(rng, extent, jnp.float32) * spread
    if len(pieces) > 0:
        entries = levels(rng, extent, pieces, -0.22, 0.18) * entries
    return jnp.clip(entries, min=-reach, max=reach).astype(held_as)


def setup_inputs(seed: int = 0) -> dict:
    keys = jax.random.split(jax.random.key(seed), 6)
    return {
        "coefficients": noise(keys[0], (K, CHARS), 1.0, 6.0, ((1, 32),)),
        "transforms": noise(keys[1], (12, J, CHARS), 1.0, 6.0, ((1, 4), (2, 8))),
        "basis": noise(keys[2], (K, 3, VERTS), K ** -0.5, 0.5, ((2, 8),)),
        "template": noise(keys[3], (3, VERTS), 1.0, 6.0, ((1, 8),)),
        "skin_weights": jnp.clip(jnp.exp(math.log(1.0) - 3.9171631 * jax.random.uniform(keys[4], (J, VERTS), jnp.float32) ** levels(keys[4], (J, VERTS), ((1, 8),), -0.2, 0.2)), 0.019897461, 1.0).astype(jnp.bfloat16),
    }


def skin_block(coefficients, joint_poses, basis_block, template_block, weight_block):
    flattened = basis_block.reshape(basis_block.shape[0], -1)
    shaped = jnp.dot(coefficients.T, flattened, preferred_element_type=jnp.float32)
    shaped = shaped + template_block.reshape(1, -1).astype(jnp.float32)
    shaped = shaped.reshape(coefficients.shape[1], 3, -1)
    blended = jnp.einsum("mjr,jv->mrv", joint_poses.astype(jnp.float32), weight_block.astype(jnp.float32))
    positions = []
    for matrix_row in range(3):
        component = blended[4 * matrix_row + 3]
        for column in range(3):
            component = component + blended[4 * matrix_row + column] * shaped[:, column, :]
        positions.append(component)
    return jnp.stack(positions, axis=1).astype(jnp.bfloat16)


def reference(coefficients, transforms, basis, template, skin_weights):
    weight_float = skin_weights.astype(jnp.float32)
    normalized = (weight_float / jnp.sum(weight_float, axis=0, keepdims=True)).astype(jnp.bfloat16)
    group_size = R * N_BATCH

    def per_group(cycle_group):
        offset = (cycle_group * group_size).astype(jnp.int32)
        group_coefficients = lax.dynamic_slice_in_dim(coefficients, offset, group_size, 1)
        group_poses = lax.dynamic_slice_in_dim(transforms, offset, group_size, 2)
        results = []
        for step_index in range(STEPS):
            block_index = jnp.mod(cycle_group - step_index, N_BLK).astype(jnp.int32)
            vertex_offset = (block_index * VB).astype(jnp.int32)
            basis_block = lax.dynamic_slice_in_dim(basis, vertex_offset, VB, 2)
            template_block = lax.dynamic_slice_in_dim(template, vertex_offset, VB, 1)
            weight_block = lax.dynamic_slice_in_dim(normalized, vertex_offset, VB, 1)
            results.append(skin_block(group_coefficients, group_poses, basis_block, template_block, weight_block))
        return jnp.stack(results, axis=1)

    stacked = lax.map(per_group, jnp.arange(N_BLK, dtype=jnp.int32))
    return stacked.reshape(N_BLK * group_size, STEPS, 3, VB)
```

```python
import functools

import jax
import jax.numpy as jnp
from jax import lax
from jax.experimental import pallas as pl
from jax.experimental.pallas import tpu as pltpu
from jax.sharding import PartitionSpec as P

STEPS = 4
CHAR_BLOCK = 128
LANES = 256


def round_up(n, multiple):
    return -(-n // multiple) * multiple


def passed_along(block, axis, distance):
    devices = range(lax.axis_size(axis))
    route = [((i - distance) % len(devices), i) for i in devices]
    return lax.ppermute(block, axis, route)


def normalize(skin_weights):
    weight_float = skin_weights.astype(jnp.float32)
    return (weight_float / jnp.sum(weight_float, axis=0, keepdims=True)).astype(jnp.bfloat16)


def skin_kernel(coef_ref, pose_ref, perm_ref, *refs, shapes):
    block_refs, out_ref, pose_rows, merged = refs[:STEPS], refs[STEPS], refs[-2], refs[-1]
    chars = coef_ref.shape[1]
    components = pose_ref.shape[1]
    joints = pose_ref.shape[0] * pose_ref.shape[2]
    group = perm_ref.shape[0] // STEPS
    coef_rows = coef_ref[...].astype(jnp.float32).T.astype(jnp.bfloat16)
    for m in range(components):
        poses = pose_ref[:, m].astype(jnp.float32).reshape(joints, chars)
        pose_rows[m * chars : (m + 1) * chars, :] = poses.T.astype(jnp.bfloat16)
    for lane in range(0, out_ref.shape[3], LANES):
        lanes = slice(lane, lane + LANES)
        for s, block in enumerate(block_refs):
            shaped = [
                jnp.dot(
                    coef_rows,
                    block[e * shapes : (e + 1) * shapes, lanes],
                    preferred_element_type=jnp.float32,
                )
                for e in range(3)
            ]
            blended = jnp.dot(
                pose_rows[...], block[3 * shapes :, lanes], preferred_element_type=jnp.float32
            )
            blended = blended.reshape(components, chars, LANES)
            for d in range(3):
                value = blended[4 * d + 3]
                for e in range(3):
                    value = value + blended[4 * d + e] * shaped[e]
                value = value.astype(jnp.bfloat16)
                for h in range(chars // group):
                    merged[d, h, s * group : (s + 1) * group, :] = value[
                        h * group : (h + 1) * group
                    ]
        for d in range(3):
            for h in range(chars // group):
                rows = jnp.dot(
                    perm_ref[...], merged[d, h], preferred_element_type=jnp.float32
                ).astype(jnp.bfloat16)
                out_ref[h * group : (h + 1) * group, d, :, lanes] = rows.reshape(
                    group, STEPS, LANES
                )


def skin(coefficients, poses, blocks, shapes):
    chars = coefficients.shape[1]
    vertices = blocks[0].shape[1]
    cb = min(CHAR_BLOCK, chars)
    group = min(256 // STEPS, cb)
    row = jnp.arange(group * STEPS)
    perm = (row[None, :] == (row % STEPS * group + row // STEPS)[:, None]).astype(jnp.bfloat16)
    joints = poses.shape[0] * poses.shape[2]
    whole = pl.BlockSpec(blocks[0].shape, lambda i: (0, 0))
    return pl.pallas_call(
        functools.partial(skin_kernel, shapes=shapes),
        grid=(chars // cb,),
        in_specs=[
            pl.BlockSpec((coefficients.shape[0], cb), lambda i: (0, i)),
            pl.BlockSpec(poses.shape[:3] + (cb,), lambda i: (0, 0, 0, i)),
            pl.BlockSpec(perm.shape, lambda i: (0, 0)),
        ]
        + [whole] * STEPS,
        out_specs=pl.BlockSpec((cb, 3, STEPS, vertices), lambda i: (i, 0, 0, 0)),
        out_shape=jax.ShapeDtypeStruct((chars, 3, STEPS, vertices), jnp.bfloat16),
        scratch_shapes=[
            pltpu.VMEM((poses.shape[1] * cb, joints), jnp.bfloat16),
            pltpu.VMEM((3, cb // group, group * STEPS, LANES), jnp.bfloat16),
        ],
        compiler_params=pltpu.CompilerParams(dimension_semantics=("arbitrary",)),
        name="skin",
    )(coefficients, poses, perm, *blocks)


def per_device(coefficients, transforms, basis, template, skin_weights):
    parts = lax.axis_size("batch")
    components, own_joints, group_chars = transforms.shape
    padded_joints = round_up(own_joints, 8)
    poses = transforms.reshape(components, own_joints, parts, group_chars // parts)
    poses = jnp.transpose(poses, (2, 0, 1, 3))
    poses = jnp.pad(poses, ((0, 0), (0, 0), (0, padded_joints - own_joints), (0, 0)))
    poses = lax.all_to_all(poses, "batch", split_axis=0, concat_axis=0)

    count, _, vertices = basis.shape
    shapes = round_up(count + 1, 16)
    spare = shapes - count - 1
    weights = normalize(skin_weights).reshape(parts, own_joints, vertices)
    weights = jnp.pad(weights, ((0, 0), (0, padded_joints - own_joints), (0, 0)))
    displacements = jnp.concatenate(
        [
            jnp.transpose(basis, (1, 0, 2)),
            template[:, None, :],
            jnp.zeros((3, spare, vertices), basis.dtype),
        ],
        axis=1,
    )
    own = jnp.concatenate(
        [displacements.reshape(-1, vertices), weights.reshape(-1, vertices)], axis=0
    )
    blocks = [own] + [passed_along(own, "blk", s) for s in range(1, STEPS)]

    ones = jnp.ones((1, coefficients.shape[1]), coefficients.dtype)
    coefficients = jnp.concatenate(
        [coefficients, ones, jnp.zeros((spare, coefficients.shape[1]), coefficients.dtype)], axis=0
    )
    out = skin(coefficients, poses, blocks, shapes)
    return jnp.transpose(out, (0, 2, 1, 3))


def solution(mesh):
    in_specs = (
        P(None, ("blk", "batch")),
        P(None, "batch", "blk"),
        P(None, None, "blk"),
        P(None, "blk"),
        P(None, "blk"),
    )
    out_specs = P(("blk", "batch"), None, None, None)
    return jax.shard_map(
        per_device, mesh=mesh, in_specs=in_specs, out_specs=out_specs, check_vma=False
    )
```

```python
import functools

import jax
import jax.numpy as jnp
from jax import lax
from jax.experimental import pallas as pl
from jax.experimental.pallas import tpu as pltpu
from jax.sharding import PartitionSpec as P

STEPS = 4
CHAR_BLOCK = 128


def round_up(n, multiple):
    return -(-n // multiple) * multiple


def passed_along(block, axis, distance):
    devices = range(lax.axis_size(axis))
    route = [((i - distance) % len(devices), i) for i in devices]
    return lax.ppermute(block, axis, route)


def swapped(half, axis):
    devices = range(lax.axis_size(axis))
    return lax.ppermute(half, axis, [(i, i ^ 1) for i in devices])


def normalize(skin_weights):
    weight_float = skin_weights.astype(jnp.float32)
    return (weight_float / jnp.sum(weight_float, axis=0, keepdims=True)).astype(jnp.bfloat16)


def rows_of(array):
    return array.astype(jnp.float32).T.astype(jnp.bfloat16)


def positions(coef_rows, pose_rows, block, shapes):
    chars = coef_rows.shape[0]
    shaped = [
        jnp.dot(
            coef_rows, block[e * shapes : (e + 1) * shapes, :], preferred_element_type=jnp.float32
        )
        for e in range(3)
    ]
    blended = jnp.dot(pose_rows, block[3 * shapes :, :], preferred_element_type=jnp.float32)
    blended = blended.reshape(-1, chars, block.shape[1])
    for d in range(3):
        value = blended[4 * d + 3]
        for e in range(3):
            value = value + blended[4 * d + e] * shaped[e]
        yield d, value.astype(jnp.bfloat16)


def first_kernel(coef_ref, pose_ref, *refs, shapes):
    halves, (coef_rows, pose_rows, out_ref) = refs[:2], refs[2:]
    chars = coef_ref.shape[1]
    joints = pose_ref.shape[0] * pose_ref.shape[2]
    coef_rows[...] = rows_of(coef_ref[...])
    for m in range(pose_ref.shape[1]):
        poses = pose_ref[:, m].astype(jnp.float32).reshape(joints, chars)
        pose_rows[0, m * chars : (m + 1) * chars, :] = rows_of(poses)
    for half, block in enumerate(halves):
        for d, value in positions(coef_rows[...], pose_rows[0], block, shapes):
            out_ref[half, d] = value


def middle_kernel(side_ref, coef_rows, pose_rows, *refs, shapes):
    halves, out_ref = refs[:2], refs[2]
    for i, block in enumerate(halves):
        half = jnp.where(side_ref[0] == i, 0, 1)
        for d, value in positions(coef_rows[...], pose_rows[0], block, shapes):
            out_ref[half, d] = value


def last_kernel(side_ref, coef_rows, pose_rows, *refs, shapes):
    halves, perm_ref, earlier, out_ref, merged = refs[:2], refs[2], refs[3:-2], refs[-2], refs[-1]
    chars = coef_rows.shape[0]
    rows = perm_ref.shape[0]
    group = rows // STEPS
    width = halves[0].shape[1]
    for i, block in enumerate(halves):
        half = jnp.where(side_ref[0] == i, 0, 1)
        lanes = pl.ds(pl.multiple_of(half * width, width), width)
        for d, value in positions(coef_rows[...], pose_rows[0], block, shapes):
            for h in range(chars // group):
                own = slice(h * group, (h + 1) * group)
                for s, ref in enumerate(earlier):
                    merged[d, h, s * group : (s + 1) * group, :] = ref[half, d, own, :]
                merged[d, h, (STEPS - 1) * group :, :] = value[own]
        for d in range(3):
            for h in range(chars // group):
                spread = jnp.dot(
                    perm_ref[...], merged[d, h], preferred_element_type=jnp.float32
                ).astype(jnp.bfloat16)
                out_ref[h * group : (h + 1) * group, d, :, lanes] = spread.reshape(
                    group, STEPS, width
                )


def skin(coefficients, poses, own, fetched, side, shapes):
    count, chars = coefficients.shape
    parts, components, joints, _ = poses.shape
    width = own[0].shape[1]
    cb = min(CHAR_BLOCK, chars)
    steps = chars // cb
    group = min(256 // STEPS, cb)
    row = jnp.arange(group * STEPS)
    perm = (row[None, :] == (row % STEPS * group + row // STEPS)[:, None]).astype(jnp.bfloat16)
    params = pltpu.CompilerParams(dimension_semantics=("arbitrary",))
    half_spec = pl.BlockSpec(own[0].shape, lambda i: (0, 0))
    side_spec = pl.BlockSpec(memory_space=pltpu.SMEM)
    row_specs = [
        pl.BlockSpec((cb, count), lambda i: (i, 0)),
        pl.BlockSpec((1, components * cb, parts * joints), lambda i: (i, 0, 0)),
    ]
    value_spec = pl.BlockSpec((2, 3, cb, width), lambda i: (0, 0, i, 0))
    value_shape = jax.ShapeDtypeStruct((2, 3, chars, width), jnp.bfloat16)
    flops = 2 * chars * 2 * width * (3 * 256 + components * 256)
    cost = pl.CostEstimate(flops=flops, transcendentals=0, bytes_accessed=6 * chars * 2 * width)
    ready = (fetched[0], swapped(fetched[0], "batch"))
    coef_rows, pose_rows, value = pl.pallas_call(
        functools.partial(first_kernel, shapes=shapes),
        grid=(steps,),
        in_specs=[
            pl.BlockSpec((count, cb), lambda i: (0, i)),
            pl.BlockSpec((parts, components, joints, cb), lambda i: (0, 0, 0, i)),
            half_spec,
            half_spec,
        ],
        out_specs=row_specs + [value_spec],
        out_shape=[
            jax.ShapeDtypeStruct((chars, count), jnp.bfloat16),
            jax.ShapeDtypeStruct((steps, components * cb, parts * joints), jnp.bfloat16),
            value_shape,
        ],
        compiler_params=params,
        cost_estimate=cost,
        name="skin_first",
    )(coefficients, poses, *own)
    values = [value]
    for half in fetched[1:]:
        block = ready
        half, values[-1] = lax.optimization_barrier((half, values[-1]))
        ready = (half, swapped(half, "batch"))
        values.append(
            pl.pallas_call(
                functools.partial(middle_kernel, shapes=shapes),
                grid=(steps,),
                in_specs=[side_spec] + row_specs + [half_spec] * 2,
                out_specs=value_spec,
                out_shape=value_shape,
                compiler_params=params,
                cost_estimate=cost,
                name="skin_middle",
            )(side, coef_rows, pose_rows, *block)
        )
    return pl.pallas_call(
        functools.partial(last_kernel, shapes=shapes),
        grid=(steps,),
        in_specs=[side_spec]
        + row_specs
        + [half_spec] * 2
        + [pl.BlockSpec(perm.shape, lambda i: (0, 0))]
        + [value_spec] * len(values),
        out_specs=pl.BlockSpec((cb, 3, STEPS, 2 * width), lambda i: (i, 0, 0, 0)),
        out_shape=jax.ShapeDtypeStruct((chars, 3, STEPS, 2 * width), jnp.bfloat16),
        scratch_shapes=[pltpu.VMEM((3, cb // group, group * STEPS, width), jnp.bfloat16)],
        compiler_params=params,
        cost_estimate=cost,
        name="skin_last",
    )(side, coef_rows, pose_rows, *ready, perm, *values)


def per_device(coefficients, transforms, basis, template, skin_weights):
    parts = lax.axis_size("batch")
    components, own_joints, group_chars = transforms.shape
    padded_joints = round_up(own_joints, 8)

    count, _, vertices = basis.shape
    shapes = round_up(count + 1, 16)
    spare = shapes - count - 1
    weights = normalize(skin_weights).reshape(parts, own_joints, vertices)
    weights = jnp.pad(weights, ((0, 0), (0, padded_joints - own_joints), (0, 0)))
    displacements = jnp.concatenate(
        [
            jnp.transpose(basis, (1, 0, 2)),
            template[:, None, :],
            jnp.zeros((3, spare, vertices), basis.dtype),
        ],
        axis=1,
    )
    own = jnp.concatenate(
        [displacements.reshape(-1, vertices), weights.reshape(-1, vertices)], axis=0
    )
    width = vertices // 2
    side = lax.axis_index("batch") % 2
    low, high = own[:, :width], own[:, width:]
    mine = jnp.where(side == 0, low, high)
    fetched = [passed_along(mine, "blk", s) for s in range(1, STEPS)]

    poses = transforms.reshape(components, own_joints, parts, group_chars // parts)
    poses = jnp.transpose(poses, (2, 0, 1, 3))
    poses = jnp.pad(poses, ((0, 0), (0, 0), (0, padded_joints - own_joints), (0, 0)))
    poses = lax.all_to_all(poses, "batch", split_axis=0, concat_axis=0)

    ones = jnp.ones((1, coefficients.shape[1]), coefficients.dtype)
    coefficients = jnp.concatenate(
        [coefficients, ones, jnp.zeros((spare, coefficients.shape[1]), coefficients.dtype)], axis=0
    )
    side = side.astype(jnp.int32).reshape(1)
    out = skin(coefficients, poses, (low, high), fetched, side, shapes)
    return jnp.transpose(out, (0, 2, 1, 3))


def solution(mesh):
    in_specs = (
        P(None, ("blk", "batch")),
        P(None, "batch", "blk"),
        P(None, None, "blk"),
        P(None, "blk"),
        P(None, "blk"),
    )
    out_specs = P(("blk", "batch"), None, None, None)
    return jax.shard_map(
        per_device, mesh=mesh, in_specs=in_specs, out_specs=out_specs, check_vma=False
    )
```

```python
import functools

import jax
import jax.numpy as jnp
from jax import lax
from jax.experimental import pallas as pl
from jax.experimental.pallas import tpu as pltpu
from jax.sharding import PartitionSpec as P

STEPS = 4
CHAR_BLOCK = 128


def round_up(n, multiple):
    return -(-n // multiple) * multiple


def passed_along(block, axis, distance):
    devices = range(lax.axis_size(axis))
    route = [((i - distance) % len(devices), i) for i in devices]
    return lax.ppermute(block, axis, route)


def swapped(half, axis):
    devices = range(lax.axis_size(axis))
    return lax.ppermute(half, axis, [(i, i ^ 1) for i in devices])


def normalize(skin_weights):
    weight_float = skin_weights.astype(jnp.float32)
    return (weight_float / jnp.sum(weight_float, axis=0, keepdims=True)).astype(jnp.bfloat16)


def rows_of(array):
    return array.astype(jnp.float32).T.astype(jnp.bfloat16)


def positions(coef_rows, pose_rows, block, shapes):
    chars = coef_rows.shape[0]
    shaped = [
        jnp.dot(
            coef_rows, block[e * shapes : (e + 1) * shapes, :], preferred_element_type=jnp.float32
        )
        for e in range(3)
    ]
    blended = jnp.dot(pose_rows, block[3 * shapes :, :], preferred_element_type=jnp.float32)
    blended = blended.reshape(-1, chars, block.shape[1])
    for d in range(3):
        value = blended[4 * d + 3]
        for e in range(3):
            value = value + blended[4 * d + e] * shaped[e]
        yield d, value.astype(jnp.bfloat16)


def spread_rows(coef_ref, pose_ref, pose_rows):
    chars = coef_ref.shape[1]
    joints = pose_ref.shape[0] * pose_ref.shape[2]
    for m in range(pose_ref.shape[1]):
        poses = pose_ref[:, m].astype(jnp.float32).reshape(joints, chars)
        pose_rows[m * chars : (m + 1) * chars, :] = rows_of(poses)
    return rows_of(coef_ref[...])


def first_kernel(coef_ref, pose_ref, low, high, out_ref, pose_rows, *, shapes):
    coef_rows = spread_rows(coef_ref, pose_ref, pose_rows)
    for half, block in enumerate((low, high)):
        for d, value in positions(coef_rows, pose_rows[...], block, shapes):
            out_ref[half, d] = value


def last_kernel(side_ref, coef_ref, pose_ref, perm_ref, first, *refs, shapes):
    blocks, out_ref, pose_rows, merged = refs[:-3], refs[-3], refs[-2], refs[-1]
    coef_rows = spread_rows(coef_ref, pose_ref, pose_rows)
    chars = coef_rows.shape[0]
    group = perm_ref.shape[0] // STEPS
    width = blocks[0].shape[1]
    for i in range(2):
        half = jnp.where(side_ref[0] == i, 0, 1)
        lanes = pl.ds(pl.multiple_of(half * width, width), width)
        for s in range(1, STEPS):
            block = blocks[2 * (s - 1) + i]
            for d, value in positions(coef_rows, pose_rows[...], block, shapes):
                for h in range(chars // group):
                    merged[d, h, s * group : (s + 1) * group, :] = value[
                        h * group : (h + 1) * group
                    ]
        for d in range(3):
            for h in range(chars // group):
                own = slice(h * group, (h + 1) * group)
                merged[d, h, :group, :] = first[half, d, own, :]
                spread = jnp.dot(
                    perm_ref[...], merged[d, h], preferred_element_type=jnp.float32
                ).astype(jnp.bfloat16)
                out_ref[own, d, :, lanes] = spread.reshape(group, STEPS, width)


def skin(coefficients, poses, own, fetched, side, shapes):
    count, chars = coefficients.shape
    parts, components, joints, _ = poses.shape
    width = own[0].shape[1]
    cb = min(CHAR_BLOCK, chars)
    group = min(256 // STEPS, cb)
    row = jnp.arange(group * STEPS)
    perm = (row[None, :] == (row % STEPS * group + row // STEPS)[:, None]).astype(jnp.bfloat16)
    params = pltpu.CompilerParams(dimension_semantics=("arbitrary",))
    half_spec = pl.BlockSpec(own[0].shape, lambda i: (0, 0))
    char_specs = [
        pl.BlockSpec((count, cb), lambda i: (0, i)),
        pl.BlockSpec((parts, components, joints, cb), lambda i: (0, 0, 0, i)),
    ]
    value_spec = pl.BlockSpec((2, 3, cb, width), lambda i: (0, 0, i, 0))
    rows_scratch = pltpu.VMEM((components * cb, parts * joints), jnp.bfloat16)
    flops = 2 * chars * 2 * width * (3 * 256 + components * 256)
    cost = pl.CostEstimate(flops=flops, transcendentals=0, bytes_accessed=6 * chars * 2 * width)
    blocks = [half for f in fetched[:-1] for half in (f, swapped(f, "batch"))]
    first = pl.pallas_call(
        functools.partial(first_kernel, shapes=shapes),
        grid=(chars // cb,),
        in_specs=char_specs + [half_spec] * 2,
        out_specs=value_spec,
        out_shape=jax.ShapeDtypeStruct((2, 3, chars, width), jnp.bfloat16),
        scratch_shapes=[rows_scratch],
        compiler_params=params,
        cost_estimate=cost,
        name="skin_first",
    )(coefficients, poses, *own)
    farthest, first = lax.optimization_barrier((fetched[-1], first))
    blocks += [farthest, swapped(farthest, "batch")]
    return pl.pallas_call(
        functools.partial(last_kernel, shapes=shapes),
        grid=(chars // cb,),
        in_specs=[pl.BlockSpec(memory_space=pltpu.SMEM)]
        + char_specs
        + [pl.BlockSpec(perm.shape, lambda i: (0, 0)), value_spec]
        + [half_spec] * len(blocks),
        out_specs=pl.BlockSpec((cb, 3, STEPS, 2 * width), lambda i: (i, 0, 0, 0)),
        out_shape=jax.ShapeDtypeStruct((chars, 3, STEPS, 2 * width), jnp.bfloat16),
        scratch_shapes=[
            rows_scratch,
            pltpu.VMEM((3, cb // group, group * STEPS, width), jnp.bfloat16),
        ],
        compiler_params=params,
        cost_estimate=cost,
        name="skin_last",
    )(side, coefficients, poses, perm, first, *blocks)


def per_device(coefficients, transforms, basis, template, skin_weights):
    parts = lax.axis_size("batch")
    components, own_joints, group_chars = transforms.shape
    padded_joints = round_up(own_joints, 8)

    count, _, vertices = basis.shape
    shapes = round_up(count + 1, 16)
    spare = shapes - count - 1
    weights = normalize(skin_weights).reshape(parts, own_joints, vertices)
    weights = jnp.pad(weights, ((0, 0), (0, padded_joints - own_joints), (0, 0)))
    displacements = jnp.concatenate(
        [
            jnp.transpose(basis, (1, 0, 2)),
            template[:, None, :],
            jnp.zeros((3, spare, vertices), basis.dtype),
        ],
        axis=1,
    )
    own = jnp.concatenate(
        [displacements.reshape(-1, vertices), weights.reshape(-1, vertices)], axis=0
    )
    width = vertices // 2
    side = lax.axis_index("batch") % 2
    low, high = own[:, :width], own[:, width:]
    mine = jnp.where(side == 0, low, high)
    fetched = [passed_along(mine, "blk", s) for s in range(1, STEPS)]

    poses = transforms.reshape(components, own_joints, parts, group_chars // parts)
    poses = jnp.transpose(poses, (2, 0, 1, 3))
    poses = jnp.pad(poses, ((0, 0), (0, 0), (0, padded_joints - own_joints), (0, 0)))
    poses = lax.all_to_all(poses, "batch", split_axis=0, concat_axis=0)

    ones = jnp.ones((1, coefficients.shape[1]), coefficients.dtype)
    coefficients = jnp.concatenate(
        [coefficients, ones, jnp.zeros((spare, coefficients.shape[1]), coefficients.dtype)], axis=0
    )
    side = side.astype(jnp.int32).reshape(1)
    out = skin(coefficients, poses, (low, high), fetched, side, shapes)
    return jnp.transpose(out, (0, 2, 1, 3))


def solution(mesh):
    in_specs = (
        P(None, ("blk", "batch")),
        P(None, "batch", "blk"),
        P(None, None, "blk"),
        P(None, "blk"),
        P(None, "blk"),
    )
    out_specs = P(("blk", "batch"), None, None, None)
    return jax.shard_map(
        per_device, mesh=mesh, in_specs=in_specs, out_specs=out_specs, check_vma=False
    )
```

```python
import functools

import jax
import jax.numpy as jnp
from jax import lax
from jax.experimental import pallas as pl
from jax.experimental.pallas import tpu as pltpu
from jax.sharding import PartitionSpec as P

STEPS = 4
CHAR_BLOCK = 128


def round_up(n, multiple):
    return -(-n // multiple) * multiple


def passed_along(block, axis, distance):
    devices = range(lax.axis_size(axis))
    route = [((i - distance) % len(devices), i) for i in devices]
    return lax.ppermute(block, axis, route)


def swapped(half, axis):
    devices = range(lax.axis_size(axis))
    return lax.ppermute(half, axis, [(i, i ^ 1) for i in devices])


def normalize(skin_weights):
    weight_float = skin_weights.astype(jnp.float32)
    return (weight_float / jnp.sum(weight_float, axis=0, keepdims=True)).astype(jnp.bfloat16)


def rows_of(array):
    return array.astype(jnp.float32).T.astype(jnp.bfloat16)


def positions(coef_rows, pose_rows, block, shapes):
    chars = coef_rows.shape[0]
    shaped = [
        jnp.dot(
            coef_rows, block[e * shapes : (e + 1) * shapes, :], preferred_element_type=jnp.float32
        )
        for e in range(3)
    ]
    blended = jnp.dot(pose_rows, block[3 * shapes :, :], preferred_element_type=jnp.float32)
    blended = blended.reshape(-1, chars, block.shape[1])
    for d in range(3):
        value = blended[4 * d + 3]
        for e in range(3):
            value = value + blended[4 * d + e] * shaped[e]
        yield d, value.astype(jnp.bfloat16)


def spread_rows(coef_ref, pose_ref, pose_rows):
    chars = coef_ref.shape[1]
    joints = pose_ref.shape[0] * pose_ref.shape[2]
    for m in range(pose_ref.shape[1]):
        poses = pose_ref[:, m].astype(jnp.float32).reshape(joints, chars)
        pose_rows[m * chars : (m + 1) * chars, :] = rows_of(poses)
    return rows_of(coef_ref[...])


def first_kernel(coef_ref, pose_ref, low, high, out_ref, pose_rows, *, shapes):
    coef_rows = spread_rows(coef_ref, pose_ref, pose_rows)
    for half, block in enumerate((low, high)):
        for d, value in positions(coef_rows, pose_rows[...], block, shapes):
            out_ref[half, d] = value


def last_kernel(side_ref, coef_ref, pose_ref, perm_ref, first, *refs, shapes):
    blocks, out_ref, pose_rows, merged = refs[:-3], refs[-3], refs[-2], refs[-1]
    coef_rows = spread_rows(coef_ref, pose_ref, pose_rows)
    chars = coef_rows.shape[0]
    group = perm_ref.shape[0] // STEPS
    width = blocks[0].shape[1]
    for i in range(2):
        half = jnp.where(side_ref[0] == i, 0, 1)
        lanes = pl.ds(pl.multiple_of(half * width, width), width)
        for s in range(1, STEPS):
            block = blocks[2 * (s - 1) + i]
            for d, value in positions(coef_rows, pose_rows[...], block, shapes):
                for h in range(chars // group):
                    merged[d, h, s * group : (s + 1) * group, :] = value[
                        h * group : (h + 1) * group
                    ]
        for d in range(3):
            for h in range(chars // group):
                own = slice(h * group, (h + 1) * group)
                merged[d, h, :group, :] = first[half, d, own, :]
                spread = jnp.dot(
                    perm_ref[...], merged[d, h], preferred_element_type=jnp.float32
                ).astype(jnp.bfloat16)
                out_ref[own, d, :, lanes] = spread.reshape(group, STEPS, width)


def skin(coefficients, poses, own, fetched, side, shapes):
    count, chars = coefficients.shape
    parts, components, joints, _ = poses.shape
    width = own[0].shape[1]
    cb = min(CHAR_BLOCK, chars)
    group = min(256 // STEPS, cb)
    row = jnp.arange(group * STEPS)
    perm = (row[None, :] == (row % STEPS * group + row // STEPS)[:, None]).astype(jnp.bfloat16)
    params = pltpu.CompilerParams(dimension_semantics=("arbitrary",))
    half_spec = pl.BlockSpec(own[0].shape, lambda i: (0, 0))
    char_specs = [
        pl.BlockSpec((count, cb), lambda i: (0, i)),
        pl.BlockSpec((parts, components, joints, cb), lambda i: (0, 0, 0, i)),
    ]
    value_spec = pl.BlockSpec((2, 3, cb, width), lambda i: (0, 0, i, 0))
    rows_scratch = pltpu.VMEM((components * cb, parts * joints), jnp.bfloat16)
    flops = 2 * chars * 2 * width * (3 * 256 + components * 256)
    cost = pl.CostEstimate(flops=flops, transcendentals=0, bytes_accessed=6 * chars * 2 * width)
    early = swapped(fetched[1], "batch")
    first = pl.pallas_call(
        functools.partial(first_kernel, shapes=shapes),
        grid=(chars // cb,),
        in_specs=char_specs + [half_spec] * 2,
        out_specs=value_spec,
        out_shape=jax.ShapeDtypeStruct((2, 3, chars, width), jnp.bfloat16),
        scratch_shapes=[rows_scratch],
        compiler_params=params,
        cost_estimate=cost,
        name="skin_first",
    )(coefficients, poses, *own)
    nearest, farthest, first = lax.optimization_barrier((fetched[0], fetched[2], first))
    blocks = [nearest, swapped(nearest, "batch"), fetched[1], early]
    blocks += [farthest, swapped(farthest, "batch")]
    return pl.pallas_call(
        functools.partial(last_kernel, shapes=shapes),
        grid=(chars // cb,),
        in_specs=[pl.BlockSpec(memory_space=pltpu.SMEM)]
        + char_specs
        + [pl.BlockSpec(perm.shape, lambda i: (0, 0)), value_spec]
        + [half_spec] * len(blocks),
        out_specs=pl.BlockSpec((cb, 3, STEPS, 2 * width), lambda i: (i, 0, 0, 0)),
        out_shape=jax.ShapeDtypeStruct((chars, 3, STEPS, 2 * width), jnp.bfloat16),
        scratch_shapes=[
            rows_scratch,
            pltpu.VMEM((3, cb // group, group * STEPS, width), jnp.bfloat16),
        ],
        compiler_params=params,
        cost_estimate=cost,
        name="skin_last",
    )(side, coefficients, poses, perm, first, *blocks)


def per_device(coefficients, transforms, basis, template, skin_weights):
    parts = lax.axis_size("batch")
    components, own_joints, group_chars = transforms.shape
    padded_joints = round_up(own_joints, 8)

    count, _, vertices = basis.shape
    shapes = round_up(count + 1, 16)
    spare = shapes - count - 1
    weights = normalize(skin_weights).reshape(parts, own_joints, vertices)
    weights = jnp.pad(weights, ((0, 0), (0, padded_joints - own_joints), (0, 0)))
    displacements = jnp.concatenate(
        [
            jnp.transpose(basis, (1, 0, 2)),
            template[:, None, :],
            jnp.zeros((3, spare, vertices), basis.dtype),
        ],
        axis=1,
    )
    own = jnp.concatenate(
        [displacements.reshape(-1, vertices), weights.reshape(-1, vertices)], axis=0
    )
    width = vertices // 2
    side = lax.axis_index("batch") % 2
    low, high = own[:, :width], own[:, width:]
    mine = jnp.where(side == 0, low, high)
    fetched = [passed_along(mine, "blk", s) for s in range(1, STEPS)]

    poses = transforms.reshape(components, own_joints, parts, group_chars // parts)
    poses = jnp.transpose(poses, (2, 0, 1, 3))
    poses = jnp.pad(poses, ((0, 0), (0, 0), (0, padded_joints - own_joints), (0, 0)))
    poses = lax.all_to_all(poses, "batch", split_axis=0, concat_axis=0)

    ones = jnp.ones((1, coefficients.shape[1]), coefficients.dtype)
    coefficients = jnp.concatenate(
        [coefficients, ones, jnp.zeros((spare, coefficients.shape[1]), coefficients.dtype)], axis=0
    )
    side = side.astype(jnp.int32).reshape(1)
    out = skin(coefficients, poses, (low, high), fetched, side, shapes)
    return jnp.transpose(out, (0, 2, 1, 3))


def solution(mesh):
    in_specs = (
        P(None, ("blk", "batch")),
        P(None, "batch", "blk"),
        P(None, None, "blk"),
        P(None, "blk"),
        P(None, "blk"),
    )
    out_specs = P(("blk", "batch"), None, None, None)
    return jax.shard_map(
        per_device, mesh=mesh, in_specs=in_specs, out_specs=out_specs, check_vma=False
    )
```
